32 devices in a mesh: exp: 8 (over z, x), dat: 4 (over y, core).
Axes of the slice: x: 2, y: 2, z: 4, core: 2. Of those that a mesh axis runs over, the one named last changes fastest.
Arguments:
- tokens: bfloat16 [4096, 1024], P(('exp', 'dat')), may hold values from -6 to 6
- norm_gain: float32 [1024], replicated, may hold values from 0.25 to 1.75
- router_weight: bfloat16 [1024, 32], P(None, 'exp'), may hold values from -0.1875 to 0.1875
- inner_weight: bfloat16 [32, 1024, 4096], P('exp', None, 'dat'), may hold values from -0.1875 to 0.1875
- outer_weight: bfloat16 [32, 4096, 1024], P('exp', 'dat'), may hold values from -0.09375 to 0.09375
- slot_tokens: int32 [32, 256], P('exp', 'dat'), may hold values from 0 to 4095, as said below
- slot_ids: int32 [4096, 2], P(('exp', 'dat')), may hold values from 0 to 8191, as said below
Outputs:
- mixed: bfloat16 [4096, 1024], P(('exp', 'dat'))
The draws below stay inside these ranges and needn't reach their ends.
Inputs may be any that keep to these rules, and one draw needn't show every extreme that they name: `slot_tokens`: column c of an expert names only tokens of the devices whose dat index is c // 64; one expert names no token twice. The 256 slots of the experts of one exp index in one dat group name tokens of any one device at most 96 times, exactly 96 times for some devices, and no times for some. Every token is named by exactly 2 slots. slot_ids[t] holds the two slots e * 256 + c with slot_tokens[e, c] = t, the smaller first.
All inputs are finite; a program needn't handle non-finite values.
Results may differ from the reference program's by a relative error of at most 0.0085.
Values may be sent and summed in bfloat16 or wider, within the bound.
No kernel may reach another device: no remote copies, remote signals or barrier semaphores. Data moves between devices by JAX's collectives and lax.ppermute only.
A program may use at most 64 MiB of HBM per device.

```python
import jax
import jax.numpy as jnp
from jax import lax

D = 1024
FF = 4096
E_DEV = 4
TOK_DEV = 128
E = 32
C_DAT = 64
CAP = 256
TOKENS = 4096
N_EXP = 8
N_DAT = 4


def build_routes(key):
    base = jax.random.fold_in(key, 7)
    groups = N_DAT
    owners = N_EXP
    tok_rows = TOK_DEV
    spread = E_DEV * C_DAT
    average = 2 * TOK_DEV // N_EXP
    ranking = jnp.arange(owners, dtype=jnp.int32)
    profile = jnp.where(ranking < owners // 8, 3 * average, jnp.where(ranking < 3 * owners // 4, average, 0)).astype(jnp.int32)
    key_shift, key_slot, key_token = jax.random.split(base, 3)
    shifts = jax.vmap(lambda subkey: jax.random.permutation(subkey, owners))(jax.random.split(key_shift, groups)).astype(jnp.int32)
    counts = profile[(ranking[None, None, :] + shifts[:, :, None]) % owners]
    after_dev = jnp.cumsum(counts, axis=1)
    start_dev = after_dev - counts
    after_own = jnp.cumsum(counts, axis=2)
    start_own = after_own - counts
    orders = jax.vmap(lambda subkey: jax.random.permutation(subkey, spread))(jax.random.split(key_slot, groups * owners)).reshape(groups, owners, spread).astype(jnp.int32)
    circuits = jax.vmap(lambda subkey: jax.random.permutation(subkey, tok_rows))(jax.random.split(key_token, groups * owners)).reshape(groups, owners, tok_rows).astype(jnp.int32)
    owner_of = jnp.sum((after_own[:, :, None, :] <= orders[:, :, :, None]).astype(jnp.int32), axis=-1)
    within = orders - jnp.take_along_axis(start_own, owner_of, axis=2)
    position = jnp.take_along_axis(start_dev, owner_of, axis=2) + within
    flat_index = (owner_of * tok_rows + position % tok_rows).reshape(groups, owners * spread)
    local_token = jnp.take_along_axis(circuits.reshape(groups, owners * tok_rows), flat_index, axis=1).reshape(groups, owners, spread)
    group_index = jnp.arange(groups, dtype=jnp.int32)[:, None, None]
    token_id = (owner_of * groups + group_index) * tok_rows + local_token
    slot_tokens = token_id.reshape(groups, owners, E_DEV, C_DAT).transpose(1, 2, 0, 3).reshape(owners * E_DEV, groups * C_DAT)
    steps_seq = jnp.arange(2 * tok_rows, dtype=jnp.int32)
    after_by_owner = after_dev.transpose(0, 2, 1)
    device_of = jnp.sum((after_by_owner[:, :, None, :] <= steps_seq[None, None, :, None]).astype(jnp.int32), axis=-1)
    within_dev = steps_seq[None, None, :] - jnp.take_along_axis(start_dev.transpose(0, 2, 1), device_of, axis=2)
    sorted_pos = jnp.take_along_axis(start_own.transpose(0, 2, 1), device_of, axis=2) + within_dev
    inverse = jnp.argsort(orders, axis=-1).astype(jnp.int32)
    flat_slot = (device_of * spread + sorted_pos).reshape(groups, owners * 2 * tok_rows)
    slot_pos = jnp.take_along_axis(inverse.reshape(groups, owners * spread), flat_slot, axis=1).reshape(groups, owners, 2 * tok_rows)
    slot_global = (device_of * E_DEV + slot_pos // C_DAT) * CAP + group_index * C_DAT + slot_pos % C_DAT
    token_place = jnp.argsort(circuits, axis=-1).astype(jnp.int32)
    earlier_id = jnp.take_along_axis(slot_global, token_place, axis=2)
    later_id = jnp.take_along_axis(slot_global, token_place + tok_rows, axis=2)
    paired = jnp.stack([jnp.minimum(earlier_id, later_id), jnp.maximum(earlier_id, later_id)], axis=-1)
    slot_ids = paired.transpose(1, 0, 2, 3).reshape(owners * groups * tok_rows, 2)
    return (slot_tokens.astype(jnp.int32), slot_ids.astype(jnp.int32))


def draw_slot_tokens(key, part):
    return build_routes(key)[0]


def draw_slot_ids(key, part):
    return build_routes(key)[1]


def shard_levels(rng, extent, cuts, smallest, high):
    factor_of, own = 1.0, jax.random.fold_in(rng, 6)
    for dim, blocks in cuts:
        draws = jnp.exp(jax.random.uniform(jax.random.fold_in(own, dim), (blocks,), jnp.float32, smallest / len(cuts), high / len(cuts)))
        factor_of = factor_of * jnp.repeat(draws, extent[dim] // blocks).reshape([-1 if axis == dim else 1 for axis in range(len(extent))])
    return factor_of


def normal_values(own_key, extent, width, bound, cuts=(), kind=jnp.bfloat16):
    values = width * jax.random.normal(own_key, extent, jnp.float32)
    if cuts:
        values = values * shard_levels(own_key, extent, cuts, -0.22, 0.18)
    return jnp.clip(values, -bound, bound).astype(kind)


def setup_inputs(seed: int = 0) -> dict:
    keys = jax.random.split(jax.random.key(seed), 8)
    tokens = normal_values(keys[0], (TOKENS, D), 1.0, 6.0, ((0, 32),))
    norm_gain = jnp.clip(1.0 + 0.15 * jax.random.normal(keys[1], (D,), jnp.float32), 0.25, 1.75)
    router_weight = normal_values(keys[2], (D, E), D ** -0.5, 0.1875, ((1, 8),))
    inner_weight = normal_values(keys[3], (E, D, FF), D ** -0.5, 0.1875, ((0, 8), (2, 4)))
    outer_weight = normal_values(keys[4], (E, FF, D), FF ** -0.5, 0.09375, ((0, 8), (1, 4)))
    slot_tokens = draw_slot_tokens(jax.random.fold_in(keys[7], 71), 0)
    slot_ids = draw_slot_ids(jax.random.fold_in(keys[7], 71), 0)
    return dict(tokens=tokens, norm_gain=norm_gain, router_weight=router_weight, inner_weight=inner_weight, outer_weight=outer_weight, slot_tokens=slot_tokens, slot_ids=slot_ids)


EPSILON = 1e-06

def reference(tokens, norm_gain, router_weight, inner_weight, outer_weight, slot_tokens, slot_ids):
    values = tokens.astype(jnp.float32)
    scale = lax.rsqrt(lax.optimization_barrier(jnp.mean(values * values, axis=-1, keepdims=True)) + EPSILON)
    normed = (values * scale * norm_gain.astype(jnp.float32)).astype(jnp.bfloat16)
    slot_rows = jnp.take(normed, slot_tokens, axis=0)
    gate_score = jax.nn.sigmoid(jnp.einsum('ecd,de->ec', slot_rows.astype(jnp.float32), router_weight.astype(jnp.float32)))
    capacity = slot_tokens.shape[1]
    ff_block = FF // N_DAT

    def expert(inputs):
        block, first_weight, second_weight = inputs
        hidden = jax.nn.relu(jnp.dot(block, first_weight, preferred_element_type=jnp.float32)).astype(jnp.bfloat16)
        pieces = hidden.reshape(capacity, N_DAT, ff_block).astype(jnp.float32)
        seconds = second_weight.reshape(N_DAT, ff_block, D).astype(jnp.float32)
        partial_sums = jnp.einsum('ckf,kfd->kcd', pieces, seconds).astype(jnp.bfloat16)
        partial_sums = lax.optimization_barrier(partial_sums)
        return lax.optimization_barrier(jnp.sum(partial_sums.astype(jnp.float32), axis=0))
    expert_out = lax.map(expert, (slot_rows, inner_weight, outer_weight))
    weighted = (gate_score[:, :, None] * expert_out).astype(jnp.bfloat16).reshape(-1, D)
    chosen = jnp.take(weighted, slot_ids.reshape(-1), axis=0).reshape(slot_ids.shape[0], 2, D).astype(jnp.float32)
    combined = chosen[:, 0] + chosen[:, 1]
    return (values + combined).astype(jnp.bfloat16)
```

```python
import functools

import jax
import jax.numpy as jnp
from jax import lax
from jax.experimental import pallas as pl
from jax.experimental.pallas import tpu as pltpu
from jax.sharding import PartitionSpec as P

EPSILON = 1e-06
CHUNKS = 2


def swap(x, axis, bit):
    size = lax.axis_size(axis)
    return lax.ppermute(x, axis, [(i, i ^ bit) for i in range(size)])


def bits_of(size):
    return [1 << b for b in reversed(range(size.bit_length() - 1))]


def spread(block, axis, bits):
    held = {0: block}
    for bit in bits:
        for mask in list(held):
            held[mask | bit] = swap(held[mask], axis, bit)
    return held


def fold(parts, axis, bits):
    for bit in bits:
        kept = {}
        for mask in sorted((m for m in parts if not m & bit), reverse=True):
            came = swap(parts[mask | bit], axis, bit).astype(jnp.float32)
            kept[mask] = parts[mask].astype(jnp.float32) + came
        last = len(kept) == 1
        parts = kept if last else {m: v.astype(jnp.bfloat16) for m, v in kept.items()}
    return parts[0]


def select_kernel(count, places, *refs):
    blocks, (mine, other), (held,) = refs[:count], refs[count:-1], refs[-1:]
    rows = blocks[0].shape[0]
    for j, block in enumerate(blocks):
        held[pl.ds(j * rows, rows), :] = block[...]
    slots, tokens = places.shape[0], held.shape[0]
    chosen = lax.broadcasted_iota(jnp.int32, (slots, tokens), 1) == places[...]
    picked = jnp.dot(chosen.astype(jnp.bfloat16), held[...], preferred_element_type=jnp.float32)
    mine[...] = picked[: slots // 2].astype(jnp.bfloat16)
    other[...] = picked[slots // 2 :].astype(jnp.bfloat16)


def select_rows(places, blocks):
    rows, width = blocks[0].shape
    slots = places.shape[0]
    tokens = rows * len(blocks)
    out = jax.ShapeDtypeStruct((slots // 2, width), jnp.bfloat16)
    return pl.pallas_call(
        functools.partial(select_kernel, len(blocks)),
        out_shape=(out, out),
        scratch_shapes=[pltpu.VMEM((tokens, width), jnp.bfloat16)],
        cost_estimate=pl.CostEstimate(
            flops=2 * slots * tokens * width, bytes_accessed=2 * width * (slots + tokens), transcendentals=0
        ),
        name="select_rows",
    )(places, *blocks)


def combine_kernel(places, mine, other, *outs):
    rows = outs[0].shape[0]
    slots = mine.shape[0]
    tokens = rows * len(outs)
    chosen = lax.broadcasted_iota(jnp.int32, (tokens, 2 * slots), 0) == places[...]
    chosen = chosen.astype(jnp.bfloat16)
    summed = jnp.dot(chosen[:, :slots], mine[...], preferred_element_type=jnp.float32)
    summed += jnp.dot(chosen[:, slots:], other[...], preferred_element_type=jnp.float32)
    for j, out in enumerate(outs):
        out[...] = summed[j * rows : (j + 1) * rows].astype(jnp.bfloat16)


def combine_rows(places, mine, other, count, rows):
    slots, width = mine.shape
    out = jax.ShapeDtypeStruct((rows, width), jnp.bfloat16)
    return pl.pallas_call(
        combine_kernel,
        out_shape=(out,) * count,
        cost_estimate=pl.CostEstimate(
            flops=4 * slots * rows * count * width,
            bytes_accessed=2 * width * (2 * slots + rows * count),
            transcendentals=0,
        ),
        name="combine_rows",
    )(places, mine, other)


def inner_kernel(lanes, chunks, *refs):
    inputs, (first, second), outs = refs[: lanes * chunks], refs[lanes * chunks :][:2], refs[lanes * chunks + 2 :]
    hidden, results, rows_in = outs[0], outs[1 : 1 + lanes], outs[-1]
    rows, width = inputs[0].shape
    for lane in range(lanes):
        for k in range(chunks):
            rows_in[pl.ds(lane * rows, rows), pl.ds(k * width, width)] = inputs[lane * chunks + k][...]
    units = first.shape[1]
    tile = min(256, units)
    for n in range(0, units, tile):
        acc = jnp.dot(rows_in[...], first[:, n : n + tile], preferred_element_type=jnp.float32)
        hidden[:, n : n + tile] = jnp.maximum(acc, 0.0).astype(jnp.bfloat16)
    outer_tiles(hidden, second, results)


def outer_kernel(hidden, second, *results):
    outer_tiles(hidden, second, results)


def outer_tiles(hidden, second, results):
    rows = results[0].shape[0]
    width = second.shape[1]
    tile = min(256, width)
    for n in range(0, width, tile):
        acc = jnp.dot(hidden[...], second[:, n : n + tile], preferred_element_type=jnp.float32)
        for lane, result in enumerate(results):
            result[:, n : n + tile] = acc[lane * rows : (lane + 1) * rows].astype(jnp.bfloat16)


def experts(inputs, first, second, lanes, chunks):
    count, full, units = first.shape
    slots, width = inputs[0].shape
    rows = slots // count
    row_spec = pl.BlockSpec((rows, width), lambda e: (e, 0))
    hidden_spec = pl.BlockSpec((rows * lanes, units), lambda e: (e, 0))
    sums = jax.ShapeDtypeStruct((slots, width), jnp.bfloat16)
    hidden = jax.ShapeDtypeStruct((slots * lanes, units), jnp.bfloat16)
    work = 2 * slots * lanes * units
    out = pl.pallas_call(
        functools.partial(inner_kernel, lanes, chunks),
        grid=(count,),
        in_specs=[row_spec] * (lanes * chunks)
        + [
            pl.BlockSpec((None, full, units), lambda e: (e, 0, 0)),
            pl.BlockSpec((None, units, width), lambda e: (e, 0, 0)),
        ],
        out_specs=[hidden_spec] + [row_spec] * lanes,
        out_shape=[hidden] + [sums] * lanes,
        scratch_shapes=[pltpu.VMEM((rows * lanes, full), jnp.bfloat16)],
        cost_estimate=pl.CostEstimate(
            flops=work * (full + width), bytes_accessed=2 * count * units * (full + width), transcendentals=0
        ),
        name="inner_and_first_chunk",
    )(*inputs, first, second)
    results = [out[1:]]
    for k in range(1, chunks):
        results.append(
            pl.pallas_call(
                outer_kernel,
                grid=(count,),
                in_specs=[hidden_spec, pl.BlockSpec((None, units, width), lambda e, k=k: (e, 0, k))],
                out_specs=[row_spec] * lanes,
                out_shape=[sums] * lanes,
                cost_estimate=pl.CostEstimate(
                    flops=work * width, bytes_accessed=2 * count * units * width, transcendentals=0
                ),
                name="later_chunk",
            )(out[0], second)
        )
    return results


def body(tokens, norm_gain, router_weight, inner_weight, outer_weight, slot_tokens, slot_ids):
    exp_count, dat_count = lax.axis_size("exp"), lax.axis_size("dat")
    tok_rows, width = tokens.shape
    experts_dev, cap_dev = slot_tokens.shape
    slots = experts_dev * cap_dev
    chunks = CHUNKS
    part = width // chunks
    exp_bits, dat_bits = bits_of(exp_count), bits_of(dat_count)
    pair_bit = 2
    line_bits = [b for b in exp_bits if b != pair_bit]
    me = lax.axis_index("exp")

    values = tokens.astype(jnp.float32)
    scale = lax.rsqrt(jnp.mean(values * values, axis=-1, keepdims=True) + EPSILON)
    columns = [slice(k * part, (k + 1) * part) for k in range(chunks)]
    normed = [(values[:, c] * scale * norm_gain[c]).astype(jnp.bfloat16) for c in columns]
    lines = [spread(rows, "exp", line_bits) for rows in normed]
    masks = list(lines[0])

    own_tokens = slot_tokens.reshape(-1)
    all_tokens = jnp.concatenate([own_tokens, swap(slot_tokens, "exp", pair_bit).reshape(-1)])
    away = (all_tokens // (tok_rows * dat_count)) ^ me
    places = jnp.full(all_tokens.shape, -1, jnp.int32)
    for j, mask in enumerate(masks):
        places = jnp.where(away == mask, j * tok_rows + all_tokens % tok_rows, places)

    slot_rows, lanes = [], []
    for line in lines:
        mine, other = select_rows(places[:, None], [line[m] for m in masks])
        rows = mine + swap(other, "exp", pair_bit)
        slot_rows.append(rows)
        lanes.append(spread(rows, "dat", dat_bits))
    lane_masks = list(lanes[0])

    logits = sum(
        jnp.dot(rows, router_weight[c], preferred_element_type=jnp.float32) for rows, c in zip(slot_rows, columns)
    )
    own_expert = lax.broadcasted_iota(jnp.int32, (slots, experts_dev), 0) // cap_dev
    here = own_expert == lax.broadcasted_iota(jnp.int32, (slots, experts_dev), 1)
    gate = jax.nn.sigmoid(jnp.sum(jnp.where(here, logits, 0.0), axis=1, keepdims=True))

    inputs = [lanes[k][m] for m in lane_masks for k in range(chunks)]
    partial = experts(inputs, inner_weight, outer_weight, len(lane_masks), chunks)

    mixed = []
    for k in range(chunks):
        summed = fold(dict(zip(lane_masks, partial[k])), "dat", dat_bits[::-1])
        weighted = (gate * summed).astype(jnp.bfloat16)
        other = swap(weighted, "exp", pair_bit)
        blocks = combine_rows(places[None, :], weighted, other, len(masks), tok_rows)
        combined = fold(dict(zip(masks, blocks)), "exp", line_bits[::-1])
        mixed.append((values[:, columns[k]] + combined).astype(jnp.bfloat16))
    return jnp.concatenate(mixed, axis=1)


def solution(mesh):
    in_specs = (
        P(("exp", "dat"), None),
        P(),
        P(None, "exp"),
        P("exp", None, "dat"),
        P("exp", "dat", None),
        P("exp", "dat"),
        P(("exp", "dat"), None),
    )
    out_specs = P(("exp", "dat"), None)
    return jax.shard_map(body, mesh=mesh, in_specs=in_specs, out_specs=out_specs, check_vma=False)
```

```python
import functools

import jax
import jax.numpy as jnp
from jax import lax
from jax.experimental import pallas as pl
from jax.experimental.pallas import tpu as pltpu
from jax.sharding import PartitionSpec as P


EPSILON = 1e-06
CHUNKS = 2
FETCH_FLOPS = 400_000_000


def swap(x, axis, bit):
    size = lax.axis_size(axis)
    return lax.ppermute(x, axis, [(i, i ^ bit) for i in range(size)])


def bits_of(size):
    return [1 << b for b in reversed(range(size.bit_length() - 1))]


def spread(block, axis, bits):
    held = {0: block}
    for bit in bits:
        for mask in list(held):
            held[mask | bit] = swap(held[mask], axis, bit)
    return held


def fold(parts, axis, bits):
    for bit in bits:
        kept = {}
        for mask in sorted((m for m in parts if not m & bit), reverse=True):
            kept[mask] = (parts[mask], swap(parts[mask | bit], axis, bit))
        if len(kept) == 1:
            return kept[0]
        parts = {m: add_rows(*pair) for m, pair in kept.items()}


def in_vmem(kernel, outs, operands, scratch=(), flops=0):
    spec = pl.BlockSpec(memory_space=pltpu.VMEM)
    moved = sum(2 * x.size for x in (*outs, *operands))
    return pl.pallas_call(
        kernel,
        in_specs=[spec] * len(operands),
        out_specs=(spec,) * len(outs),
        out_shape=tuple(pltpu.VMEM(x.shape, x.dtype) for x in outs),
        scratch_shapes=scratch,
        cost_estimate=pl.CostEstimate(flops=flops, bytes_accessed=moved, transcendentals=0),
        compiler_params=pltpu.CompilerParams(vmem_limit_bytes=12 << 20),
    )(*(pltpu.with_memory_space_constraint(x, pltpu.VMEM) for x in operands))


def fetch_kernel(source, target, sems):
    count = source.shape[0]
    copies = [pltpu.make_async_copy(source.at[e], target.at[e], sems.at[e]) for e in range(count)]
    for copy in copies:
        copy.start()
    for copy in copies:
        copy.wait()


def fetch(array):
    spec = pl.BlockSpec(memory_space=pltpu.HBM)
    return pl.pallas_call(
        fetch_kernel,
        in_specs=[spec],
        out_specs=pl.BlockSpec(memory_space=pltpu.VMEM),
        out_shape=pltpu.VMEM(array.shape, array.dtype),
        scratch_shapes=[pltpu.SemaphoreType.DMA((array.shape[0],))],
        cost_estimate=pl.CostEstimate(flops=FETCH_FLOPS, bytes_accessed=4 * array.size, transcendentals=0),
        compiler_params=pltpu.CompilerParams(vmem_limit_bytes=1 << 20),
        name="fetch",
    )(pltpu.with_memory_space_constraint(array, pltpu.HBM))


def norm_kernel(tokens_hbm, gain_hbm, *refs):
    *outs, tokens, gain, sems = refs
    copies = [
        pltpu.make_async_copy(tokens_hbm, tokens, sems.at[0]),
        pltpu.make_async_copy(gain_hbm, gain, sems.at[1]),
    ]
    for copy in copies:
        copy.start()
    for copy in copies:
        copy.wait()
    values = tokens[...].astype(jnp.float32)
    scale = lax.rsqrt(jnp.mean(values * values, axis=-1, keepdims=True) + EPSILON)
    normed = (values * scale * gain[...]).astype(jnp.bfloat16)
    width = outs[0].shape[1]
    for k, out in enumerate(outs):
        out[...] = normed[:, k * width : (k + 1) * width]


def add_kernel(one, two, out):
    out[...] = (one[...].astype(jnp.float32) + two[...].astype(jnp.float32)).astype(out.dtype)


def add_rows(one, two):
    (out,) = in_vmem(add_kernel, (one,), (one, two))
    return out


def weigh_kernel(gate, one, two, out):
    summed = one[...].astype(jnp.float32) + two[...].astype(jnp.float32)
    out[...] = (gate[:, :1] * summed).astype(out.dtype)


def gate_kernel(cap, router, *refs):
    rows, gate = refs[:-1], refs[-1]
    width = rows[0].shape[1]
    logits = 0.0
    for k, block in enumerate(rows):
        logits += lax.dot_general(
            block[...],
            router[:, k * width : (k + 1) * width],
            (((1,), (1,)), ((), ())),
            preferred_element_type=jnp.float32,
        )
    own = lax.broadcasted_iota(jnp.int32, logits.shape, 0) // cap
    here = own == lax.broadcasted_iota(jnp.int32, logits.shape, 1)
    score = jax.nn.sigmoid(jnp.sum(jnp.where(here, logits, 0.0), axis=1, keepdims=True))
    gate[...] = jnp.broadcast_to(score, gate.shape)


def finish_kernel(tokens, *refs):
    pieces, out = refs[:-1], refs[-1]
    width = pieces[0].shape[1]
    for k in range(len(pieces) // 2):
        cols = slice(k * width, (k + 1) * width)
        summed = pieces[2 * k][...].astype(jnp.float32) + pieces[2 * k + 1][...].astype(jnp.float32)
        out[:, cols] = (tokens[:, cols].astype(jnp.float32) + summed).astype(out.dtype)


def route_kernel(masks, tok_rows, dat_count, mine, other, column, row, wanted):
    count, cap = mine.shape
    for e in range(count):
        wanted[:, e * cap : (e + 1) * cap] = mine[e : e + 1, :]
        wanted[:, (count + e) * cap : (count + e + 1) * cap] = other[e : e + 1, :]
    tokens = wanted[...]
    away = (tokens // (tok_rows * dat_count)) ^ lax.axis_index("exp")
    places = jnp.full(tokens.shape, -1, jnp.int32)
    for j, mask in enumerate(masks):
        places = jnp.where(away == mask, j * tok_rows + tokens % tok_rows, places)
    row[...] = places
    column[...] = jnp.broadcast_to(places, (column.shape[1], column.shape[0])).T


def select_kernel(count, places, *refs):
    blocks, (mine, other), (held,) = refs[:count], refs[count:-1], refs[-1:]
    rows = blocks[0].shape[0]
    for j, block in enumerate(blocks):
        held[pl.ds(j * rows, rows), :] = block[...]
    slots, lanes = places.shape
    which = lax.broadcasted_iota(jnp.int32, (slots, lanes), 1)
    chosen = [(which + j * lanes == places[...]).astype(jnp.bfloat16) for j in range(held.shape[0] // lanes)]
    picked = jnp.dot(jnp.concatenate(chosen, axis=1), held[...], preferred_element_type=jnp.float32)
    mine[...] = picked[: slots // 2].astype(jnp.bfloat16)
    other[...] = picked[slots // 2 :].astype(jnp.bfloat16)


def select_rows(places, blocks):
    rows, width = blocks[0].shape
    slots = places.shape[0]
    tokens = rows * len(blocks)
    out = jax.ShapeDtypeStruct((slots // 2, width), jnp.bfloat16)
    return in_vmem(
        functools.partial(select_kernel, len(blocks)),
        (out, out),
        (places, *blocks),
        [pltpu.VMEM((tokens, width), jnp.bfloat16)],
        2 * slots * tokens * width,
    )


def combine_kernel(places, mine, other, *outs):
    rows = outs[0].shape[0]
    slots = mine.shape[0]
    tokens = rows * len(outs)
    chosen = lax.broadcasted_iota(jnp.int32, (tokens, 2 * slots), 0) == places[...]
    chosen = chosen.astype(jnp.bfloat16)
    summed = jnp.dot(chosen[:, :slots], mine[...], preferred_element_type=jnp.float32)
    summed += jnp.dot(chosen[:, slots:], other[...], preferred_element_type=jnp.float32)
    for j, out in enumerate(outs):
        out[...] = summed[j * rows : (j + 1) * rows].astype(jnp.bfloat16)


def combine_rows(places, mine, other, count, rows):
    slots, width = mine.shape
    out = jax.ShapeDtypeStruct((rows, width), jnp.bfloat16)
    return in_vmem(combine_kernel, (out,) * count, (places, mine, other), (), 4 * slots * rows * count * width)


def inner_kernel(lanes, k, last, *refs):
    inputs, first, out, rows_in = refs[:lanes], refs[-3], refs[-2], refs[-1]
    before = refs[lanes] if k else None
    width = inputs[0].shape[1]
    count = first.shape[0]
    rows = inputs[0].shape[0] // count

    @pl.loop(0, count)
    def _(e):
        for lane in range(lanes):
            rows_in[pl.ds(lane * rows, rows), :] = inputs[lane][pl.ds(e * rows, rows), :]
        acc = jnp.dot(rows_in[...], first[e, k * width : (k + 1) * width, :], preferred_element_type=jnp.float32)
        if before is not None:
            acc += before[e]
        out[e] = jnp.maximum(acc, 0.0).astype(out.dtype) if last else acc


def outer_kernel(k, hidden, second, *results):
    slots, width = results[0].shape
    count = hidden.shape[0]
    rows = slots // count

    @pl.loop(0, count)
    def _(e):
        acc = jnp.dot(hidden[e], second[e, :, k * width : (k + 1) * width], preferred_element_type=jnp.float32)
        for lane, result in enumerate(results):
            result[pl.ds(e * rows, rows), :] = acc[lane * rows : (lane + 1) * rows].astype(jnp.bfloat16)


def body(tokens, norm_gain, router_weight, inner_weight, outer_weight, slot_tokens, slot_ids):
    exp_count, dat_count = lax.axis_size("exp"), lax.axis_size("dat")
    tok_rows, width = tokens.shape
    experts_dev, cap_dev = slot_tokens.shape
    units = inner_weight.shape[2]
    slots = experts_dev * cap_dev
    chunks = CHUNKS
    part = width // chunks
    exp_bits, dat_bits = bits_of(exp_count), bits_of(dat_count)
    pair_bit = 2
    line_bits = [b for b in exp_bits if b != pair_bit]

    def shaped(*shape, dtype=jnp.bfloat16):
        return jax.ShapeDtypeStruct(shape, dtype)

    hbm, vmem = pl.BlockSpec(memory_space=pltpu.HBM), pl.BlockSpec(memory_space=pltpu.VMEM)
    normed = pl.pallas_call(
        norm_kernel,
        in_specs=[hbm, hbm],
        out_specs=(vmem,) * chunks,
        out_shape=(pltpu.VMEM((tok_rows, part), jnp.bfloat16),) * chunks,
        scratch_shapes=[
            pltpu.VMEM((tok_rows, width), jnp.bfloat16),
            pltpu.VMEM((1, width), jnp.float32),
            pltpu.SemaphoreType.DMA((2,)),
        ],
        compiler_params=pltpu.CompilerParams(vmem_limit_bytes=12 << 20),
        name="norm",
    )(*(pltpu.with_memory_space_constraint(x, pltpu.HBM) for x in (tokens, norm_gain[None, :])))
    lines = [spread(rows, "exp", line_bits) for rows in normed]
    masks = list(lines[0])

    column, row = in_vmem(
        functools.partial(route_kernel, tuple(masks), tok_rows, dat_count),
        (shaped(2 * slots, 128, dtype=jnp.int32), shaped(1, 2 * slots, dtype=jnp.int32)),
        (slot_tokens, swap(slot_tokens, "exp", pair_bit)),
        [pltpu.VMEM((1, 2 * slots), jnp.int32)],
    )

    slot_rows, lanes = [], []
    for line in lines:
        mine, other = select_rows(column, [line[m] for m in masks])
        rows = add_rows(mine, swap(other, "exp", pair_bit))
        slot_rows.append(rows)
        lanes.append(spread(rows, "dat", dat_bits))
    lane_masks = list(lanes[0])

    first, second = fetch(inner_weight), fetch(outer_weight)

    (gate,) = in_vmem(
        functools.partial(gate_kernel, cap_dev), (shaped(slots, 128, dtype=jnp.float32),), (router_weight.T, *slot_rows)
    )

    count = len(lane_masks)
    rows = cap_dev * count
    hidden = None
    for k in range(chunks):
        last = k == chunks - 1
        (hidden,) = in_vmem(
            functools.partial(inner_kernel, count, k, last),
            (shaped(experts_dev, rows, units, dtype=jnp.bfloat16 if last else jnp.float32),),
            (*lanes[k].values(), *([hidden] if k else []), first),
            [pltpu.VMEM((rows, part), jnp.bfloat16)],
            2 * slots * count * units * part,
        )

    pieces = []
    for k in range(chunks):
        sums = in_vmem(
            functools.partial(outer_kernel, k),
            (shaped(slots, part),) * count,
            (hidden, second),
            (),
            2 * slots * count * units * part,
        )
        pair = fold(dict(zip(lane_masks, sums)), "dat", dat_bits[::-1])
        (weighted,) = in_vmem(weigh_kernel, (shaped(slots, part),), (gate, *pair))
        other = swap(weighted, "exp", pair_bit)
        blocks = combine_rows(row, weighted, other, len(masks), tok_rows)
        pieces += fold(dict(zip(masks, blocks)), "exp", line_bits[::-1])

    return pl.pallas_call(
        finish_kernel,
        in_specs=[vmem] * (1 + len(pieces)),
        out_shape=shaped(tok_rows, width),
        compiler_params=pltpu.CompilerParams(vmem_limit_bytes=12 << 20),
        name="finish",
    )(*(pltpu.with_memory_space_constraint(x, pltpu.VMEM) for x in (tokens, *pieces)))


def solution(mesh):
    in_specs = (
        P(("exp", "dat"), None),
        P(),
        P(None, "exp"),
        P("exp", None, "dat"),
        P("exp", "dat", None),
        P("exp", "dat"),
        P(("exp", "dat"), None),
    )
    out_specs = P(("exp", "dat"), None)
    return jax.shard_map(body, mesh=mesh, in_specs=in_specs, out_specs=out_specs, check_vma=False)
```
